16 devices in a mesh: rep: 1, dp: 16 (over x, y, z, core).
Axes of the slice: x: 2, y: 2, z: 2, core: 2. Of those that a mesh axis runs over, the one named last changes fastest.
Arguments:
- x: bfloat16 [16, 2048, 640], P(('rep', 'dp'))
- dy: bfloat16 [16, 2048, 640], P(('rep', 'dp'))
- wq: bfloat16 [2, 640, 1024], replicated
- wk: bfloat16 [2, 640, 128], replicated
- wv: bfloat16 [2, 640, 128], replicated
- wo: bfloat16 [2, 1024, 640], replicated
- w_gate: bfloat16 [2, 640, 3200], replicated
- w_up: bfloat16 [2, 640, 3200], replicated
- w_down: bfloat16 [2, 3200, 640], replicated
- m_wq: float32 [2, 640, 1024], P(None, 'dp')
- m_wk: float32 [2, 640, 128], P(None, 'dp')
- m_wv: float32 [2, 640, 128], P(None, 'dp')
- m_wo: float32 [2, 1024, 640], P(None, 'dp')
- m_w_gate: float32 [2, 640, 3200], P(None, 'dp')
- m_w_up: float32 [2, 640, 3200], P(None, 'dp')
- m_w_down: float32 [2, 3200, 640], P(None, 'dp')
- v_wq: float32 [2, 640, 1024], P(None, 'dp')
- v_wk: float32 [2, 640, 128], P(None, 'dp')
- v_wv: float32 [2, 640, 128], P(None, 'dp')
- v_wo: float32 [2, 1024, 640], P(None, 'dp')
- v_w_gate: float32 [2, 640, 3200], P(None, 'dp')
- v_w_up: float32 [2, 640, 3200], P(None, 'dp')
- v_w_down: float32 [2, 3200, 640], P(None, 'dp')
Outputs:
- output 1: bfloat16 [2, 640, 1024], P('rep')
- output 2: bfloat16 [2, 640, 128], P('rep')
- output 3: bfloat16 [2, 640, 128], P('rep')
- output 4: bfloat16 [2, 1024, 640], P('rep')
- output 5: bfloat16 [2, 640, 3200], P('rep')
- output 6: bfloat16 [2, 640, 3200], P('rep')
- output 7: bfloat16 [2, 3200, 640], P('rep')
- output 8: float32 [2, 640, 1024], P('rep', 'dp')
- output 9: float32 [2, 640, 128], P('rep', 'dp')
- output 10: float32 [2, 640, 128], P('rep', 'dp')
- output 11: float32 [2, 1024, 640], P('rep', 'dp')
- output 12: float32 [2, 640, 3200], P('rep', 'dp')
- output 13: float32 [2, 640, 3200], P('rep', 'dp')
- output 14: float32 [2, 3200, 640], P('rep', 'dp')
- output 15: float32 [2, 640, 1024], P('rep', 'dp')
- output 16: float32 [2, 640, 128], P('rep', 'dp')
- output 17: float32 [2, 640, 128], P('rep', 'dp')
- output 18: float32 [2, 1024, 640], P('rep', 'dp')
- output 19: float32 [2, 640, 3200], P('rep', 'dp')
- output 20: float32 [2, 640, 3200], P('rep', 'dp')
- output 21: float32 [2, 3200, 640], P('rep', 'dp')
All inputs are finite; a program needn't handle non-finite values.
Results may differ from the reference program's by a relative error of at most 0.0255.
Values are sent between devices in bfloat16 or wider.
A program may use at most 2 GiB of HBM per device.

```python
import jax
import jax.numpy as jnp
from jax import lax

SEQUENCES = 16
TOKENS = 2048
D = 640
HEADS = 8
KV_HEADS = 1
HEAD = 128
FF = 3200
LAYERS = 2
THETA = 10000
NAMES = ("wq", "wk", "wv", "wo", "w_gate", "w_up", "w_down")
SHAPES = {
    "wq": (LAYERS, D, HEADS * HEAD),
    "wk": (LAYERS, D, KV_HEADS * HEAD),
    "wv": (LAYERS, D, KV_HEADS * HEAD),
    "wo": (LAYERS, HEADS * HEAD, D),
    "w_gate": (LAYERS, D, FF),
    "w_up": (LAYERS, D, FF),
    "w_down": (LAYERS, FF, D),
}


def bump(key, n, height):
    away = (jnp.arange(n, dtype=jnp.int32) - jax.random.randint(key, (), 0, n, jnp.int32)) % n
    return jnp.where(away < n // 8, height, 1.0)


def together(key, own, strength):
    shared = jax.random.normal(key, own.shape[1:], jnp.float32)
    return (own + strength * shared) * lax.rsqrt(1 + strength * strength)


def setup_inputs(seed: int = 0, part: int = 0) -> dict:
    kx, kdy, ka, kb, kz, kf, kh, kl, *keys = jax.random.split(jax.random.key(seed), 8 + 3 * len(NAMES))
    kx, kdy, ka, kb = (jax.random.fold_in(k, part) for k in (kx, kdy, ka, kb))
    kw, km, kv = (keys[i::3] for i in range(3))
    shape = (SEQUENCES, TOKENS, D)
    much_x, much_dy = jax.random.uniform(kz, (2,), jnp.float32, 0.0, 1.0)
    loud = 2.0 ** jax.random.uniform(jax.random.fold_in(kz, 1), (), jnp.float32, -1.0, 2.0)
    layers = 2.0 ** jax.random.uniform(kl, (LAYERS, 1, 1), jnp.float32, -1.0, 1.0)
    times = {"wq": 1.0, "wk": 1.0, "wv": 2.0, "wo": layers, "w_gate": 1.0, "w_up": bump(kh, FF, 4.0), "w_down": layers}
    x = together(ka, jax.random.normal(kx, shape, jnp.float32), much_x) * bump(kf, D, 4.0)
    dy = together(kb, jax.random.normal(kdy, shape, jnp.float32), much_dy)
    drawn = {"x": x.astype(jnp.bfloat16), "dy": (loud * dy * (SEQUENCES * TOKENS) ** -0.5).astype(jnp.bfloat16)}
    for key, name in zip(kw, NAMES, strict=True):
        drawn[name] = (jax.random.normal(key, SHAPES[name], jnp.float32) * SHAPES[name][1] ** -0.5 * times[name]).astype(jnp.bfloat16)
    for key, name in zip(km, NAMES, strict=True):
        drawn[f"m_{name}"] = 0.1 * jax.random.normal(key, SHAPES[name], jnp.float32)
    for key, name in zip(kv, NAMES, strict=True):
        drawn[f"v_{name}"] = jax.random.uniform(key, SHAPES[name], jnp.float32, 0.02, 0.06)
    return drawn


def matmul(a, w):
    return jnp.dot(a, w, preferred_element_type=jnp.float32).astype(jnp.bfloat16)


def normed(h):
    wide = h.astype(jnp.float32)
    scale = lax.rsqrt(jnp.mean(wide**2, -1, keepdims=True) + 1e-6)
    return (wide * scale).astype(jnp.bfloat16)


def turned(t, theta):
    half = t.shape[-1] // 2
    angle = jnp.arange(t.shape[0], dtype=jnp.float32)[:, None] * theta ** (-jnp.arange(half, dtype=jnp.float32) / half)
    cos, sin = jnp.cos(angle)[:, None], jnp.sin(angle)[:, None]
    a, b = t[..., :half].astype(jnp.float32), t[..., half:].astype(jnp.float32)
    return jnp.concatenate([a * cos - b * sin, b * cos + a * sin], -1).astype(jnp.bfloat16)


def seen_by(q, k, v):
    tokens, kv = q.shape[0], k.shape[1]
    q = q.reshape(tokens, kv, -1, q.shape[-1])
    scores = jnp.einsum("tgsd,ugd->gstu", q.astype(jnp.float32), k.astype(jnp.float32)) * q.shape[-1] ** -0.5
    place = jnp.arange(tokens)
    weights = jax.nn.softmax(jnp.where(place[:, None] >= place, scores, -jnp.inf), -1).astype(jnp.bfloat16)
    return jnp.einsum("gstu,ugd->tgsd", weights.astype(jnp.float32), v.astype(jnp.float32)).astype(jnp.bfloat16).reshape(tokens, -1)


def layer(h, w):
    a = normed(h)
    q, k = (turned(matmul(a, w[name]).reshape(h.shape[0], -1, HEAD), THETA) for name in ("wq", "wk"))
    h = h + matmul(seen_by(q, k, matmul(a, w["wv"]).reshape(h.shape[0], -1, HEAD)), w["wo"])
    b = normed(h)
    gate = jnp.dot(b, w["w_gate"], preferred_element_type=jnp.float32)
    up = jnp.dot(b, w["w_up"], preferred_element_type=jnp.float32)
    return h + matmul((jax.nn.silu(gate) * up).astype(jnp.bfloat16), w["w_down"])


def adamw(w, m, v, g):
    m = 0.9 * m + 0.1 * g
    v = 0.95 * v + 0.05 * g * g
    step = m * lax.rsqrt(v + 1e-8) + 0.1 * w
    return (w - 0.02 * step).astype(jnp.bfloat16), m, v


def clipped(gradients, sum_of_squares, count):
    factor = jnp.minimum(1.0, 0.5 * lax.rsqrt(sum_of_squares / count + 1e-30))
    return [g * factor for g in gradients]


def stack(weights, h):
    return lax.scan(lambda h, w: (layer(h, w), None), h, weights)[0]


def reference(x, dy, wq, wk, wv, wo, w_gate, w_up, w_down, m_wq, m_wk, m_wv, m_wo, m_w_gate, m_w_up, m_w_down, v_wq, v_wk, v_wv, v_wo, v_w_gate, v_w_up, v_w_down):
    weights = dict(zip(NAMES, (wq, wk, wv, wo, w_gate, w_up, w_down), strict=True))

    def take(so_far, sequence):
        h, by_y = sequence
        _, back = jax.vjp(stack, weights, h)
        by_weights, by_h = back(by_y)
        return jax.tree.map(lambda total, term: total + term.astype(jnp.float32), so_far, by_weights), by_h

    none_yet = {name: jnp.zeros(w.shape, jnp.float32) for name, w in weights.items()}
    by_weights, by_x = lax.scan(take, none_yet, (x, dy))
    gradients = [by_weights[name].astype(jnp.bfloat16).astype(jnp.float32) for name in NAMES]
    gradients = clipped(gradients, sum(jnp.sum(g * g) for g in gradients), sum(g.size for g in gradients))
    first = (m_wq, m_wk, m_wv, m_wo, m_w_gate, m_w_up, m_w_down)
    second = (v_wq, v_wk, v_wv, v_wo, v_w_gate, v_w_up, v_w_down)
    new = [adamw(weights[name].astype(jnp.float32), m, v, g) for name, m, v, g in zip(NAMES, first, second, gradients, strict=True)]
    return tuple(one[which] for which in range(3) for one in new)
```

```python
import functools

import jax
import jax.numpy as jnp
from jax import lax
from jax.experimental import pallas as pl
from jax.experimental.pallas import tpu as pltpu
from jax.sharding import PartitionSpec as P

HEAD = 128
THETA = 10000
NAMES = ("wq", "wk", "wv", "wo", "w_gate", "w_up", "w_down")
NEG = -1e30
HIDDEN = 2 * NEG
LOG2E = 1.4426950408889634
VMEM = 60 * 2**20
BF, F32 = jnp.bfloat16, jnp.float32


def _dot(a, b, ca=1, cb=0):
    return lax.dot_general(a, b, (((ca,), (cb,)), ((), ())), preferred_element_type=F32)


def _params(*kinds, **more):
    return pltpu.CompilerParams(dimension_semantics=kinds or None, vmem_limit_bytes=VMEM, **more)


def _cost(flops, *arrays, exps=0):
    return pl.CostEstimate(flops=int(flops), transcendentals=int(exps), bytes_accessed=int(sum(a.size * a.dtype.itemsize for a in arrays)))


def _scale(wide):
    return lax.rsqrt(jnp.mean(wide**2, -1, keepdims=True) + 1e-6)


def _normed(h):
    wide = h.astype(F32)
    return (wide * _scale(wide)).astype(BF)


def _norm_back(h, by):
    wide, by = h.astype(F32), by.astype(F32)
    r = _scale(wide)
    inner = jnp.mean(by * wide, -1, keepdims=True)
    return (by * r - wide * (r * r * r * inner)).astype(BF)


def _turn(t, cos, sin):
    return (t * cos + pltpu.roll(t, HEAD // 2, 1) * sin).astype(BF)


def _qkv_kernel(h_ref, wq_ref, wkv_ref, cos_ref, sin_ref, q_ref, k_ref, v_ref):
    a = _normed(h_ref[...])
    cos, sin = cos_ref[...], sin_ref[...]
    q = _dot(a, wq_ref[...]).astype(BF).astype(F32)
    for n in range(q.shape[1] // HEAD):
        at = slice(n * HEAD, (n + 1) * HEAD)
        q_ref[:, at] = _turn(q[:, at], cos, sin)
    kv = _dot(a, wkv_ref[...]).astype(BF)
    k_ref[...] = _turn(kv[:, :HEAD].astype(F32), cos, sin)
    v_ref[...] = kv[:, HEAD:]


def qkv(h, wq, wkv, cos, sin, block=512):
    s, d = h.shape
    row = lambda n: pl.BlockSpec((block, n), lambda i: (i, 0))
    whole = lambda a: pl.BlockSpec(a.shape, lambda i: (0, 0))
    outs = [jax.ShapeDtypeStruct((s, n), BF) for n in (wq.shape[1], HEAD, HEAD)]
    return pl.pallas_call(
        _qkv_kernel,
        grid=(s // block,),
        in_specs=[row(d), whole(wq), whole(wkv), row(HEAD), row(HEAD)],
        out_specs=[row(wq.shape[1]), row(HEAD), row(HEAD)],
        out_shape=outs,
        compiler_params=_params("arbitrary"),
        cost_estimate=_cost(2 * s * d * (wq.shape[1] + 2 * HEAD), h, wq, wkv, cos, sin, *outs),
        name="qkv",
    )(h, wq, wkv, cos, sin)


def _attend_kernel(q_ref, k_ref, v_ref, o_ref, lse_ref, top_s, mix_s, *, bk):
    bq, heads, d = q_ref.shape[0], q_ref.shape[1] // HEAD, HEAD
    scale = d**-0.5
    e = scale * LOG2E
    iq = pl.program_id(0)
    top_s[...] = jnp.full(top_s.shape, NEG, F32)
    mix_s[...] = jnp.zeros(mix_s.shape, F32)
    ones = jnp.ones((8, bk), BF)

    def block(j, masked):
        here = pl.ds(pl.multiple_of(j * bk, bk), bk)
        keys = k_ref[here, :]
        values = jnp.concatenate([v_ref[here, :].T, ones], axis=0)
        scores = [_dot(keys, q_ref[:, n * d : (n + 1) * d], 1, 1) for n in range(heads)]
        if masked:
            ok = lax.broadcasted_iota(jnp.int32, (bk, bq), 1) - lax.broadcasted_iota(jnp.int32, (bk, bq), 0) >= j * bk - iq * bq
        weights, keeps = [], []
        for n, s in enumerate(scores):
            if masked:
                s = jnp.where(ok, s, HIDDEN)
            old = top_s[n : n + 1, :]
            top = jnp.maximum(old, s.max(axis=0, keepdims=True))
            top_s[n : n + 1, :] = top
            weights.append(jnp.exp2((s - top) * e).astype(BF))
            keeps.append(jnp.exp2((old - top) * e))
        for n, (p, keep) in enumerate(zip(weights, keeps)):
            mix_s[n] = mix_s[n] * keep + _dot(values, p)

    full = lax.div(iq * bq, bk)
    last = lax.div(iq * bq + bq - 1, bk) + 1
    lax.fori_loop(0, full, lambda j, _: block(j, False), None)
    lax.fori_loop(full, last, lambda j, _: block(j, True), None)
    for n in range(heads):
        total = mix_s[n, d : d + 1, :]
        o_ref[:, n * d : (n + 1) * d] = (mix_s[n, :d, :] * (1 / total)).T.astype(BF)
        lse_ref[n : n + 1, :] = top_s[n : n + 1, :] * scale + jnp.log(total)


def attend(q, k, v, bq=512, bk=512):
    s, width = q.shape
    heads = width // HEAD
    whole = pl.BlockSpec((s, HEAD), lambda i: (0, 0))
    return pl.pallas_call(
        functools.partial(_attend_kernel, bk=bk),
        grid=(s // bq,),
        in_specs=[pl.BlockSpec((bq, width), lambda i: (i, 0)), whole, whole],
        out_specs=[pl.BlockSpec((bq, width), lambda i: (i, 0)), pl.BlockSpec((heads, bq), lambda i: (0, i))],
        out_shape=[jax.ShapeDtypeStruct((s, width), BF), jax.ShapeDtypeStruct((heads, s), F32)],
        scratch_shapes=[pltpu.VMEM((heads, bq), F32), pltpu.VMEM((heads, HEAD + 8, bq), F32)],
        compiler_params=_params("arbitrary"),
        cost_estimate=_cost(4 * s * s * width, q, k, v, q, exps=heads * s * s),
        name="attend",
    )(q, k, v)


def _attend_back_kernel(q_ref, k_ref, v_ref, do_ref, lse_ref, delta_ref, dq_ref, dk_ref, dv_ref, dq_s, dk_s, dv_s, *, bk, pair):
    bq, heads, d = q_ref.shape[0], q_ref.shape[1] // HEAD, HEAD
    scale = d**-0.5
    e = scale * LOG2E
    iq = pl.program_id(0)
    wide = pair * bq
    pieces = range(heads // pair)

    @pl.when(iq == 0)
    def _():
        dk_s[...] = jnp.zeros_like(dk_s)
        dv_s[...] = jnp.zeros_like(dv_s)

    dq_s[...] = jnp.zeros_like(dq_s)
    rows = lambda ref, i: jnp.concatenate([ref[n : n + 1, :] for n in range(i * pair, (i + 1) * pair)], axis=1)
    side = lambda ref, i: jnp.concatenate([ref[:, n * d : (n + 1) * d] for n in range(i * pair, (i + 1) * pair)], axis=0)
    lses = [rows(lse_ref, i) * LOG2E for i in pieces]
    deltas = [rows(delta_ref, i) for i in pieces]

    def block(j, masked):
        here = pl.ds(pl.multiple_of(j * bk, bk), bk)
        keys, values = k_ref[here, :], v_ref[here, :]
        qs = [side(q_ref, i) for i in pieces]
        dos = [side(do_ref, i) for i in pieces]
        scores = [_dot(keys, x, 1, 1) for x in qs]
        dps = [_dot(values, x, 1, 1) for x in dos]
        if masked:
            gap = lax.rem(lax.broadcasted_iota(jnp.int32, (bk, wide), 1), bq) - lax.broadcasted_iota(jnp.int32, (bk, wide), 0)
            ok = gap >= j * bk - iq * bq
        for n in pieces:
            p = jnp.exp2(scores[n] * e - lses[n])
            if masked:
                p = jnp.where(ok, p, 0.0)
            ds = (p * (dps[n] - deltas[n])).astype(BF)
            dv_s[here, :] += _dot(p.astype(BF), dos[n])
            dk_s[here, :] += _dot(ds, qs[n])
            dq_s[:, n * wide : (n + 1) * wide] += _dot(keys.T, ds)

    full = lax.div(iq * bq, bk)
    last = lax.div(iq * bq + bq - 1, bk) + 1
    lax.fori_loop(0, full, lambda j, _: block(j, False), None)
    lax.fori_loop(full, last, lambda j, _: block(j, True), None)
    for n in range(heads):
        dq_ref[:, n * d : (n + 1) * d] = (dq_s[:, n * bq : (n + 1) * bq] * scale).T.astype(BF)

    @pl.when(iq == pl.num_programs(0) - 1)
    def _():
        dk_ref[...] = (dk_s[...] * scale).astype(BF)
        dv_ref[...] = dv_s[...].astype(BF)


def attend_back(q, k, v, do, lse, delta, bq=256, bk=512):
    s, width = q.shape
    heads = width // HEAD
    queries = pl.BlockSpec((bq, width), lambda i: (i, 0))
    whole = pl.BlockSpec((s, HEAD), lambda i: (0, 0))
    stats = pl.BlockSpec((heads, bq), lambda i: (0, i))
    return pl.pallas_call(
        functools.partial(_attend_back_kernel, bk=bk, pair=512 // bq),
        grid=(s // bq,),
        in_specs=[queries, whole, whole, queries, stats, stats],
        out_specs=[queries, whole, whole],
        out_shape=[jax.ShapeDtypeStruct((s, width), BF)] + [jax.ShapeDtypeStruct((s, HEAD), BF)] * 2,
        scratch_shapes=[pltpu.VMEM((HEAD, heads * bq), F32), pltpu.VMEM((s, HEAD), F32), pltpu.VMEM((s, HEAD), F32)],
        compiler_params=_params("arbitrary"),
        cost_estimate=_cost(10 * s * s * width, q, q, q, k, v, exps=heads * s * s),
        name="attend_back",
    )(q, k, v, do, lse, delta)


def _join_kernel(h_ref, o_ref, wo_ref, h2_ref):
    h2_ref[...] = h_ref[...] + _dot(o_ref[...], wo_ref[...]).astype(BF)


def join(h, o, wo, block=1024):
    s, d = h.shape
    row = lambda n: pl.BlockSpec((block, n), lambda i: (i, 0))
    return pl.pallas_call(
        _join_kernel,
        grid=(s // block,),
        in_specs=[row(d), row(o.shape[1]), pl.BlockSpec(wo.shape, lambda i: (0, 0))],
        out_specs=row(d),
        out_shape=jax.ShapeDtypeStruct((s, d), BF),
        compiler_params=_params("arbitrary"),
        cost_estimate=_cost(2 * s * d * o.shape[1], h, h, o, wo),
        name="join",
    )(h, o, wo)


def _silu(g):
    s = 1 / (1 + jnp.exp2(g * -LOG2E))
    return s, g * s


def _cuts(n, wide):
    return [slice(a, min(a + wide, n)) for a in range(0, n, wide)]


def _forward_kernel(h_ref, o_ref, wo_ref, wg_ref, wu_ref, wd_ref, h2_ref, h3_ref):
    h2 = h_ref[...] + _dot(o_ref[...], wo_ref[...]).astype(BF)
    h2_ref[...] = h2
    b = _normed(h2)
    acts = []
    for at in _cuts(wg_ref.shape[1], 1280):
        _, g = _silu(_dot(b, wg_ref[:, at]))
        acts.append((g * _dot(b, wu_ref[:, at])).astype(BF))
    h3_ref[...] = h2 + _dot(jnp.concatenate(acts, axis=1), wd_ref[...]).astype(BF)


def forward(h, o, wo, wg, wu, wd, block=512):
    s, d = h.shape
    row = lambda n: pl.BlockSpec((block, n), lambda i: (i, 0))
    whole = lambda a: pl.BlockSpec(a.shape, lambda i: (0, 0), pipeline_mode=pl.Buffered(1))
    return pl.pallas_call(
        _forward_kernel,
        grid=(s // block,),
        in_specs=[row(d), row(o.shape[1]), whole(wo), whole(wg), whole(wu), whole(wd)],
        out_specs=[row(d), row(d)],
        out_shape=[jax.ShapeDtypeStruct((s, d), BF)] * 2,
        compiler_params=_params("arbitrary"),
        cost_estimate=_cost(2 * s * d * (o.shape[1] + 3 * wg.shape[1]), h, h, h, o, wo, wg, wu, wd, exps=s * wg.shape[1]),
        name="forward",
    )(h, o, wo, wg, wu, wd)


def _ffn_back_kernel(h2_ref, dy_ref, wg_ref, wu_ref, wd_ref, dh_ref, gg_ref, gu_ref, gd_ref, b_s, bt_s, dyt_s, dg_s, du_s, act_s, sg_s, su_s, *, rows):
    step = pl.program_id(0)
    s = h2_ref.shape[0]

    @pl.when(step == 0)
    def _():
        for at in _cuts(s, rows):
            b = _normed(h2_ref[at, :])
            b_s[at, :] = b
            bt_s[:, at] = b.T
            dyt_s[:, at] = dy_ref[at, :].T
        sg_s[...] = jnp.zeros_like(sg_s)
        su_s[...] = jnp.zeros_like(su_s)

    def part(i, _):
        at = pl.ds(pl.multiple_of(i * rows, rows), rows)
        b = b_s[at, :]
        gate, up = _dot(b, wg_ref[...]), _dot(b, wu_ref[...])
        by = _dot(dy_ref[at, :], wd_ref[...], 1, 1).astype(BF).astype(F32)
        sig, soft = _silu(gate)
        act_s[at, :] = (soft * up).astype(BF)
        by_up = (by * soft).astype(BF)
        by_gate = (by * up * (sig + soft * (1 - sig))).astype(BF)
        du_s[at, :] = by_up
        dg_s[at, :] = by_gate
        sg_s[at, :] += _dot(by_gate, wg_ref[...], 1, 1)
        su_s[at, :] += _dot(by_up, wu_ref[...], 1, 1)

    lax.fori_loop(0, s // rows, part, None)
    share = lambda x, ref: x.astype(BF).reshape(ref.shape)
    gg_ref[...] = share(_dot(bt_s[...], dg_s[...]), gg_ref)
    gu_ref[...] = share(_dot(bt_s[...], du_s[...]), gu_ref)
    gd_ref[...] = _dot(dyt_s[...], act_s[...]).T.astype(BF)

    @pl.when(step == pl.num_programs(0) - 1)
    def _():
        for at in _cuts(s, rows):
            by_b = (sg_s[at, :].astype(BF) + su_s[at, :].astype(BF)).astype(BF)
            dh_ref[at, :] = dy_ref[at, :] + _norm_back(h2_ref[at, :], by_b)


def ffn_back(h2, dy, wg, wu, wd, n, rows=512):
    s, d = h2.shape
    f = wg.shape[1]
    whole = pl.BlockSpec((s, d), lambda i: (0, 0), pipeline_mode=pl.Buffered(1))
    cols = pl.BlockSpec((d, d), lambda i: (0, i))
    down = pl.BlockSpec((d, d), lambda i: (i, 0))
    cut = pl.BlockSpec((n, None, d // n, d), lambda i: (0, i, 0, 0))
    cut_shape = jax.ShapeDtypeStruct((n, f // d, d // n, d), BF)
    token = lambda dt: pltpu.VMEM((s, d), dt)
    return pl.pallas_call(
        functools.partial(_ffn_back_kernel, rows=rows),
        grid=(f // d,),
        in_specs=[whole, whole, cols, cols, down],
        out_specs=[pl.BlockSpec((s, d), lambda i: (0, 0)), cut, cut, down],
        out_shape=[jax.ShapeDtypeStruct((s, d), BF), cut_shape, cut_shape, jax.ShapeDtypeStruct((f, d), BF)],
        scratch_shapes=[token(BF), pltpu.VMEM((d, s), BF), pltpu.VMEM((d, s), BF), token(BF), token(BF), token(BF), token(F32), token(F32)],
        compiler_params=_params("arbitrary"),
        cost_estimate=_cost(16 * s * d * f, h2, h2, h2, wg, wu, wd, wg, wu, wd, exps=s * f),
        name="ffn_back",
    )(h2, dy, wg, wu, wd)


def _wo_back_kernel(dh_ref, o_ref, wo_ref, do_ref, delta_ref, g_ref, acc_s):
    step = pl.program_id(0)
    dh, o = dh_ref[...], o_ref[...]
    do = _dot(dh, wo_ref[...], 1, 1).astype(BF)
    do_ref[...] = do
    for n in range(o.shape[1] // HEAD):
        at = slice(n * HEAD, (n + 1) * HEAD)
        delta_ref[n : n + 1, :] = (do[:, at].astype(F32) * o[:, at].astype(F32)).T.sum(axis=0, keepdims=True)
    new = _dot(o, dh, 0, 0)

    @pl.when(step == 0)
    def _():
        acc_s[...] = new

    @pl.when(step > 0)
    def _():
        acc_s[...] += new

    @pl.when(step == pl.num_programs(0) - 1)
    def _():
        g_ref[...] = acc_s[...].astype(BF)


def wo_back(dh, o, wo, block=1024):
    s, d = dh.shape
    width = o.shape[1]
    row = lambda n: pl.BlockSpec((block, n), lambda i: (i, 0))
    same = pl.BlockSpec(wo.shape, lambda i: (0, 0))
    heads = width // HEAD
    return pl.pallas_call(
        _wo_back_kernel,
        grid=(s // block,),
        in_specs=[row(d), row(width), same],
        out_specs=[row(width), pl.BlockSpec((heads, block), lambda i: (0, i)), same],
        out_shape=[jax.ShapeDtypeStruct((s, width), BF), jax.ShapeDtypeStruct((heads, s), F32), jax.ShapeDtypeStruct(wo.shape, BF)],
        scratch_shapes=[pltpu.VMEM(wo.shape, F32)],
        compiler_params=_params("arbitrary"),
        cost_estimate=_cost(4 * s * d * width, dh, o, o, wo, wo),
        name="wo_back",
    )(dh, o, wo)


def _qkv_back_kernel(h_ref, dq_ref, dk_ref, dv_ref, cos_ref, sin_ref, *rest, last):
    if last:
        (g_ref, acc_s), dh_ref = rest, None
    else:
        dh2_ref, wq_ref, wk_ref, wv_ref, dh_ref, g_ref, acc_s = rest
    step = pl.program_id(0)
    h = h_ref[...]
    a = _normed(h)
    cos, sin = cos_ref[...], -sin_ref[...]
    heads = [slice(n * HEAD, (n + 1) * HEAD) for n in range(dq_ref.shape[1] // HEAD)]
    dq = jnp.concatenate([_turn(dq_ref[:, at].astype(F32), cos, sin) for at in heads], axis=1)
    dk = _turn(dk_ref[...].astype(F32), cos, sin)
    dv = dv_ref[...]
    new = _dot(a, jnp.concatenate([dq, dk, dv], axis=1), 0, 0)

    @pl.when(step == 0)
    def _():
        acc_s[...] = new

    @pl.when(step > 0)
    def _():
        acc_s[...] += new

    if not last:
        by = _dot(dk, wk_ref[...], 1, 1).astype(BF) + _dot(dv, wv_ref[...], 1, 1).astype(BF)
        by = by + _dot(dq, wq_ref[...], 1, 1).astype(BF)
        dh_ref[...] = dh2_ref[...] + _norm_back(h, by)

    @pl.when(step == pl.num_programs(0) - 1)
    def _():
        d = h_ref.shape[1]
        for j in range(acc_s.shape[1] // d):
            g_ref[:, j] = acc_s[:, j * d : (j + 1) * d].astype(BF).reshape(g_ref.shape[0], d // g_ref.shape[0], d)


def qkv_back(h, dq, dk, dv, cos, sin, n, more=(), block=1024):
    s, d = h.shape
    width = dq.shape[1]
    row = lambda k: pl.BlockSpec((block, k), lambda i: (i, 0))
    whole = lambda a: pl.BlockSpec(a.shape, lambda i: (0, 0))
    total = width + 2 * HEAD
    shape = (n, total // d, d // n, d)
    in_specs = [row(d), row(width), row(HEAD), row(HEAD), row(HEAD), row(HEAD)]
    out_specs, outs = [pl.BlockSpec(shape, lambda i: (0, 0, 0, 0))], [jax.ShapeDtypeStruct(shape, BF)]
    if more:
        in_specs += [row(d)] + [whole(w) for w in more[1:]]
        out_specs, outs = [row(d)] + out_specs, [jax.ShapeDtypeStruct((s, d), BF)] + outs
    return pl.pallas_call(
        functools.partial(_qkv_back_kernel, last=not more),
        grid=(s // block,),
        in_specs=in_specs,
        out_specs=out_specs,
        out_shape=outs,
        scratch_shapes=[pltpu.VMEM((d, total), F32)],
        compiler_params=_params("arbitrary"),
        cost_estimate=_cost(2 * s * d * total * (2 if more else 1), h, dq, dk, dv, cos, sin, *outs),
        name="qkv_back",
    )(h, dq, dk, dv, cos, sin, *more)


def angles(tokens):
    half = HEAD // 2
    angle = jnp.arange(tokens, dtype=F32)[:, None] * THETA ** (-jnp.arange(half, dtype=F32) / half)
    cos, sin = jnp.cos(angle), jnp.sin(angle)
    return jnp.concatenate([cos, cos], 1), jnp.concatenate([-sin, sin], 1)


def layers_step(x, dy, weights, n):
    wq, wk, wv, wo, wg, wu, wd = weights
    layers = wq.shape[0]
    cos, sin = angles(x.shape[0])
    h, kept = x, []
    for i in range(layers):
        q, k, v = qkv(h, wq[i], jnp.concatenate([wk[i], wv[i]], 1), cos, sin)
        o, lse = attend(q, k, v)
        if i < layers - 1:
            h2, h3 = forward(h, o, wo[i], wg[i], wu[i], wd[i])
        else:
            h2, h3 = join(h, o, wo[i]), None
        kept.append((h, q, k, v, o, lse, h2))
        h = h3
    grads = [None] * layers
    for i in reversed(range(layers)):
        h, q, k, v, o, lse, h2 = kept[i]
        dh2, gg, gu, gd = ffn_back(h2, dy, wg[i], wu[i], wd[i], n)
        do, delta, go = wo_back(dh2, o, wo[i])
        dq, dk, dv = attend_back(q, k, v, do, lse, delta)
        if i:
            dy, gq = qkv_back(h, dq, dk, dv, cos, sin, n, (dh2, wq[i], wk[i], wv[i]))
        else:
            (gq,) = qkv_back(h, dq, dk, dv, cos, sin, n)
        grads[i] = (gq, go, gg, gu, gd)
    return grads


def _greet(me, offsets):
    barrier = pltpu.get_barrier_semaphore()
    for d in offsets:
        pl.semaphore_signal(barrier, inc=1, device_id={"dp": jnp.bitwise_xor(me, d)}, device_id_type=pl.DeviceIdType.MESH)
    pl.semaphore_wait(barrier, len(offsets))


def _remote(src, dst, send, recv, peer):
    return pltpu.make_async_remote_copy(src_ref=src, dst_ref=dst, send_sem=send, recv_sem=recv, device_id={"dp": peer}, device_id_type=pl.DeviceIdType.MESH)


def _squares(g):
    g = g.astype(F32)
    rows = (g * g).reshape(g.shape[0] // 8, 8, g.shape[1]).sum(axis=0)
    return sum(rows[:, a : a + 128] for a in range(0, g.shape[1], 128))


def _sum_kernel(last_ref, first_ref, rest_ref, g_ref, sq_ref, here_s, part_s, tiles_s, send, recv, send_sq, recv_sq, *, n):
    me = lax.axis_index("dp")
    others = range(1, n)
    _greet(me, others)
    copies = []
    for d in others:
        peer = jnp.bitwise_xor(me, d)
        copies.append(_remote(last_ref.at[peer], here_s.at[d], send.at[d], recv.at[d], peer))
        copies[-1].start()
    tile = _squares(first_ref[...]) + _squares(rest_ref[...])
    total = last_ref[me].astype(F32)
    for d, copy in zip(others, copies):
        copy.wait_recv()
        total += here_s[d].astype(F32)
    total = total.astype(BF)
    tile = tile + _squares(total)
    part_s[...] = tile
    tiles_s[me] = tile
    at = total.shape[0]
    g_ref[0, :at, :] = total
    g_ref[0, at:, :] = rest_ref[...]
    g_ref[1] = first_ref[...]
    squares = []
    for d in others:
        peer = jnp.bitwise_xor(me, d)
        squares.append(_remote(part_s, tiles_s.at[me], send_sq.at[d], recv_sq.at[d], peer))
        squares[-1].start()
    for copy in squares:
        copy.wait_recv()
    whole = tiles_s[0]
    for i in range(1, n):
        whole += tiles_s[i]
    sq_ref[...] = jnp.broadcast_to(jnp.sum(whole, keepdims=True), sq_ref.shape)
    for copy in copies + squares:
        copy.wait_send()


def sum_tail(last, first, rest):
    n, rows, d = last.shape
    vmem = pl.BlockSpec(memory_space=pltpu.VMEM)
    return pl.pallas_call(
        functools.partial(_sum_kernel, n=n),
        in_specs=[vmem] * 3,
        out_specs=[vmem] * 2,
        out_shape=[jax.ShapeDtypeStruct((2, first.shape[0], d), BF), jax.ShapeDtypeStruct((8, 128), F32)],
        scratch_shapes=[pltpu.VMEM((n, rows, d), BF), pltpu.VMEM((8, 128), F32), pltpu.VMEM((n, 8, 128), F32)]
        + [pltpu.SemaphoreType.DMA((n,))] * 4,
        compiler_params=pltpu.CompilerParams(collective_id=1, has_side_effects=True, vmem_limit_bytes=VMEM),
        cost_estimate=_cost(10**7, last),
        name="sum_tail",
    )(last, first, rest)


def _pieces(shapes, n):
    (d, width), (_, kv) = shapes[0], shapes[1]
    r = d // n
    out, at = [[] for _ in shapes], 0
    starts = {0: 0, 1: width, 2: width + kv}
    for j in range((width + 2 * kv) // d):
        for i, first in starts.items():
            lo, hi = max(first, j * d), min(first + shapes[i][1], (j + 1) * d)
            if lo < hi:
                out[i].append((at, lo - j * d, 0, lo - first, r, hi - lo))
        at += r
    out[3].append((at, 0, 0, 0, shapes[3][0] // n, d))
    at += shapes[3][0] // n
    for i in (4, 5):
        for j in range(shapes[i][1] // d):
            out[i].append((at, 0, 0, j * d, r, d))
            at += r
    out[6].append((at, 0, 0, 0, shapes[6][0] // n, d))
    return out, at + shapes[6][0] // n


def _adamw_kernel(me_ref, g_ref, sq_ref, *refs, pieces, count):
    w, m, v, (new,), new_m, new_v = refs[:7], refs[7:14], refs[14:21], refs[21:22], refs[22:29], refs[29:36]
    factor = jnp.minimum(1.0, 0.5 * lax.rsqrt(sq_ref[0:1, 0:1] / count + 1e-30))
    for i, places in enumerate(pieces):
        for row, col, to_row, to_col, rows, cols in places:
            src = (0, slice(row, row + rows), slice(col, col + cols))
            at = (0, slice(to_row, to_row + rows), slice(to_col, to_col + cols))
            g = g_ref[src].astype(F32) * factor
            first = 0.9 * m[i][at] + 0.1 * g
            second = 0.95 * v[i][at] + 0.05 * g * g
            old = w[i][at].astype(F32)
            new_m[i][at] = first
            new_v[i][at] = second
            new[src] = (old - 0.02 * (first * lax.rsqrt(second + 1e-8) + 0.1 * old)).astype(BF)


def adamw(me, g, squares, weights, m, v, n):
    layers = g.shape[0]
    pieces, rows = _pieces([w.shape[1:] for w in weights], n)
    shard = lambda a: pl.BlockSpec((1,) + a.shape[1:], lambda i, _: (i, 0, 0))
    mine = lambda a, w: pl.BlockSpec((1,) + a.shape[1:], lambda i, me: (i, me[0], 0))
    count = sum(w.size for w in weights)
    outs = [jax.ShapeDtypeStruct(g.shape, BF)] + [jax.ShapeDtypeStruct(a.shape, F32) for a in (*m, *v)]
    got = pl.pallas_call(
        functools.partial(_adamw_kernel, pieces=pieces, count=count),
        grid_spec=pltpu.PrefetchScalarGridSpec(
            num_scalar_prefetch=1,
            grid=(layers,),
            in_specs=[shard(g), pl.BlockSpec((8, 128), lambda i, _: (0, 0))] + [mine(a, w) for a, w in zip(m, weights)] + [shard(a) for a in (*m, *v)],
            out_specs=[shard(a) for a in outs],
        ),
        out_shape=outs,
        compiler_params=_params("arbitrary"),
        cost_estimate=_cost(20 * g.size, g, *m, *v, *m, *v),
        name="adamw",
    )(me, g, squares, *weights, *m, *v)
    return got[0], got[1:8], got[8:15]


def _gather_kernel(w_ref, out_ref, own, send, recv, send_core, recv_core, *, parts):
    me = lax.axis_index("dp")
    axes = (8, 4, 2)
    _greet(me, (*axes, 1))
    rows = w_ref.shape[0] // parts
    order = [[axes[(p + s) % 3] for s in range(3)] for p in range(parts)]
    cut = lambda p: pl.ds(p * rows, rows)

    def block(p, q):
        off = 0
        for s in range(3):
            off ^= order[p][s] if q >> s & 1 else 0
        return jnp.bitwise_xor(me, off)

    mine = pltpu.make_async_copy(w_ref, out_ref.at[me], own)
    mine.start()
    sends = []

    def pass_on(p, q):
        who = block(p, q)
        src = w_ref.at[cut(p)] if q == 0 else out_ref.at[who, cut(p)]
        first = q.bit_length()
        for s in range(first, 3):
            sends.append(_remote(src, out_ref.at[who, cut(p)], send.at[p, q | 1 << s], recv.at[p, q | 1 << s], jnp.bitwise_xor(me, order[p][s])))
            sends[-1].start()
        sends.append(_remote(src, out_ref.at[who, cut(p)], send_core.at[p, q], recv_core.at[p, q], jnp.bitwise_xor(me, 1)))
        sends[-1].start()

    def arrival(p, q, sem, other):
        slot = out_ref.at[jnp.bitwise_xor(block(p, q), other), cut(p)]
        return _remote(slot, slot, send.at[p, 0], sem.at[p, q], jnp.bitwise_xor(me, 1))

    for p in range(parts):
        pass_on(p, 0)
    for q in range(1, 8):
        for p in range(parts):
            arrival(p, q, recv, 0).wait_recv()
            pass_on(p, q)
    for q in range(8):
        for p in range(parts):
            arrival(p, q, recv_core, 1).wait_recv()
    for copy in sends:
        copy.wait_send()
    mine.wait()


def gather(w, n, parts=3):
    hbm = pl.BlockSpec(memory_space=pl.ANY)
    return pl.pallas_call(
        functools.partial(_gather_kernel, parts=parts),
        in_specs=[pl.BlockSpec(memory_space=pltpu.VMEM)],
        out_specs=hbm,
        out_shape=jax.ShapeDtypeStruct((n, *w.shape), w.dtype),
        scratch_shapes=[pltpu.SemaphoreType.DMA] + [pltpu.SemaphoreType.DMA((parts, 8))] * 4,
        compiler_params=pltpu.CompilerParams(collective_id=2, has_side_effects=True, vmem_limit_bytes=VMEM),
        cost_estimate=_cost(10**8, w),
        name="gather",
    )(w)


def _lay_out_kernel(w_ref, *outs, pieces, per):
    for l in range(outs[0].shape[0]):
        for out, places in zip(outs, pieces):
            for row, col, to_row, to_col, rows, cols in places:
                out[l, to_row : to_row + rows, to_col : to_col + cols] = w_ref[0, l * per + row : l * per + row + rows, col : col + cols]


def lay_out(gathered, shapes):
    n, rows, d = gathered.shape
    pieces, per = _pieces([s[1:] for s in shapes], n)
    return pl.pallas_call(
        functools.partial(_lay_out_kernel, pieces=pieces, per=per),
        grid=(n,),
        in_specs=[pl.BlockSpec((1, rows, d), lambda i: (i, 0, 0))],
        out_specs=[pl.BlockSpec((s[0], s[1] // n, s[2]), lambda i: (0, i, 0)) for s in shapes],
        out_shape=[jax.ShapeDtypeStruct(s, BF) for s in shapes],
        compiler_params=_params("arbitrary"),
        cost_estimate=_cost(10**6, gathered, gathered),
        name="lay_out",
    )(gathered)


def solution(mesh):
    n = mesh.shape["dp"]

    def scattered(*parts):
        return lax.psum_scatter(jnp.concatenate(parts, axis=1), "dp", scatter_dimension=0, tiled=True)[0]

    def step(x, dy, *arrays):
        weights, m, v = (arrays[i : i + 7] for i in (0, 7, 14))
        d = x.shape[2]
        blocks = lambda g: g.reshape(n, -1, d)
        grads = [[blocks(g) for g in layer] for layer in layers_step(x[0], dy[0], weights, n)]
        first = scattered(*grads[1])
        rest = scattered(*grads[0][1:])
        g, squares = sum_tail(grads[0][0], first, rest)
        me = lax.axis_index("dp").astype(jnp.int32).reshape(1)
        new, new_m, new_v = adamw(me, g, squares, weights, m, v, n)
        whole = lay_out(gather(new.reshape(-1, d), n), [w.shape for w in weights])
        return (*whole, *new_m, *new_v)

    states, all_of, cut = P(("rep", "dp"), None, None), P(None, None, None), P(None, "dp", None)
    return jax.shard_map(
        step,
        mesh=mesh,
        in_specs=(states, states) + (all_of,) * 7 + (cut,) * 14,
        out_specs=(P("rep", None, None),) * 7 + (P("rep", "dp", None),) * 14,
        check_vma=False,
    )
```
